32 devices in a mesh: dp: 4 (over y, core), tensor: 8 (over z, x).
Axes of the slice: x: 2, y: 2, z: 4, core: 2. Of those that a mesh axis runs over, the one named last changes fastest.
Arguments:
- tokens: bfloat16 [512, 1024], P('dp', 'tensor'), may hold values from -6 to 6
- init_noise: float32 [512, 1024], P('dp', 'tensor'), may hold values from -1 to 1
- segment_ids: int32 [512], P('dp'), may hold values from 0 to 7, never falling along the last dimension, each value on 1 to 256 neighbouring positions
- target: float32 [512, 1024], P('dp', 'tensor'), may hold values from -6 to 6
- norm_gain: float32 [1024], replicated, may hold values from 0.1 to 1.9
- weight_in: bfloat16 [1024, 32768], P(None, 'tensor'), may hold values from -0.1875 to 0.1875
- weight_out: bfloat16 [32768, 1024], P('tensor'), may hold values from -0.03125 to 0.03125
- moment_in: float32 [1024, 32768], P('dp', 'tensor'), may hold values from -1.5 to 1.5
- moment_out: float32 [32768, 1024], P('tensor', 'dp'), may hold values from -1.5 to 1.5
Outputs:
- new_weight_in: bfloat16 [1024, 32768], P('dp', 'tensor')
- new_weight_out: bfloat16 [32768, 1024], P('tensor', 'dp')
- new_moment_in: float32 [1024, 32768], P('dp', 'tensor')
- new_moment_out: float32 [32768, 1024], P('tensor', 'dp')
- perturbation: float32 [512, 1024], P('dp', 'tensor')
The draws below stay inside these ranges and needn't reach their ends.
Inputs may be any that keep to these rules, and one draw needn't show every extreme that they name: `segment_ids`: example ids never fall along the tokens; every example holds 1 to 256 tokens.
All inputs are finite; a program needn't handle non-finite values.
Results may differ from the reference program's by a relative error of at most 0.0051.
Values may be sent and summed in bfloat16 or wider, within the bound.
A program may use at most 128 MiB of HBM per device.

```python
import math
import jax
import jax.numpy as jnp
import numpy as np
from jax import lax

D = 1024
FF = 32768
ASCENTS = 2
TOKENS = 512
EXAMPLES = 8
MOST = 256
N_TENSOR = 8


def shard_levels(key, shape, cuts, least, high):
    def one(axis_at, blocks):
        steps = jax.random.uniform(jax.random.fold_in(jax.random.fold_in(key, 6), axis_at), (blocks,), jnp.float32, least / len(cuts), high / len(cuts))
        return jnp.repeat(jnp.exp(steps), shape[axis_at] // blocks).reshape((-1,) + (1,) * (len(shape) - axis_at - 1))

    gain = one(*cuts[0])
    for cut in cuts[1:]:
        gain = gain * one(*cut)
    return gain


def length_profile(number_of, total, limit, skew):
    weights = [(1 << 20) // math.isqrt(grade ** skew) + 1 for grade in range(2, number_of + 1)]
    surplus, given = total - limit - (number_of - 1), [1] * (number_of - 1)
    while surplus > 0:
        movable = [i for i in range(number_of - 1) if given[i] < limit]
        whole, remaining = sum([weights[i] for i in movable]), surplus
        for i in movable:
            more = min(limit - given[i], max(1, remaining * weights[i] // whole), surplus)
            given[i] = given[i] + more
            surplus = surplus - more
    return np.array([limit] + given)


def uneven(own_key, count, total, most, slope):
    if count == 2:
        one = jax.random.randint(own_key, (), max(1, total - most), min(most, total - 1) + 1)
        return jnp.stack([one, total - one])
    sizes = jnp.asarray(length_profile(count, total, most, slope), jnp.int32)
    couples = (count - 1) // 2
    giver, taker = sizes[1:1 + 2 * couples:2], sizes[2:2 + 2 * couples:2]
    room = jnp.minimum(giver - 1, most - taker)
    shifted = jax.random.randint(jax.random.fold_in(own_key, 1), (couples,), 0, 1 << 20) % (room + 1)
    sizes = sizes.at[1:1 + 2 * couples:2].set(giver - shifted).at[2:2 + 2 * couples:2].set(taker + shifted)
    return sizes[jax.random.permutation(jax.random.fold_in(own_key, 2), count)]


def scatter_about(stream_key, shape, width, most, pieces=(), held_as=jnp.bfloat16):
    gain = shard_levels(stream_key, shape, pieces, -0.22, 0.18) if pieces else 1.0
    result = jax.random.normal(stream_key, shape, jnp.float32) * width * gain
    return jnp.minimum(jnp.maximum(result, -most), most).astype(held_as)


def setup_inputs(seed: int = 0) -> dict:
    seeds = jax.random.split(jax.random.key(seed), 10)
    return {
        "tokens": scatter_about(seeds[0], (TOKENS, D), 1.0, 6.0, ((0, 4), (1, 8))),
        "init_noise": jnp.clip(jax.random.uniform(seeds[1], (TOKENS, D), jnp.float32, -1.0, 1.0) * shard_levels(seeds[1], (TOKENS, D), ((0, 4), (1, 8)), -0.4, 0.0), -1.0, 1.0),
        "segment_ids": jnp.searchsorted(jnp.cumsum(uneven(seeds[2], EXAMPLES, TOKENS, MOST, 1)), jnp.arange(TOKENS), side="right").astype(jnp.int32),
        "target": scatter_about(seeds[3], (TOKENS, D), 1.0, 6.0, ((0, 4), (1, 8)), jnp.float32),
        "norm_gain": jnp.clip(1.0 + 0.18 * jax.random.normal(seeds[4], (D,), jnp.float32), 0.1, 1.9),
        "weight_in": scatter_about(seeds[5], (D, FF), D ** -0.5, 0.1875, ((1, 8),)),
        "weight_out": scatter_about(seeds[6], (FF, D), FF ** -0.5, 0.03125, ((0, 8),)),
        "moment_in": scatter_about(seeds[7], (D, FF), 0.1, 1.5, ((0, 4), (1, 8)), jnp.float32),
        "moment_out": scatter_about(seeds[8], (FF, D), 0.1, 1.5, ((0, 8), (1, 4)), jnp.float32),
    }


coeff = 0.7978845608
adv_init = 0.5
adv_step = 0.5
decay = 0.9
learn_rate = 0.01

def gelu_value(values):
    tangent = jnp.tanh(coeff * (values + 0.044715 * values * values * values))
    return 0.5 * values * (1.0 + tangent)

def gelu_slope(values):
    tangent = jnp.tanh(coeff * (values + 0.044715 * values * values * values))
    return 0.5 * (1.0 + tangent) + 0.5 * values * (1.0 - tangent * tangent) * coeff * (1.0 + 3.0 * 0.044715 * values * values)

def reference(tokens, init_noise, segment_ids, target, norm_gain, weight_in, weight_out, moment_in, moment_out):
    block = FF // N_TENSOR
    loss_scale = 1.0 / math.sqrt(TOKENS)
    weights_in = weight_in.reshape(D, N_TENSOR, block).transpose(1, 0, 2)
    weights_out = weight_out.reshape(N_TENSOR, block, D)
    labels = jnp.arange(EXAMPLES, dtype=jnp.int32)
    onehot = (segment_ids[:, None] == labels[None, :]).astype(jnp.float32)
    counts = lax.optimization_barrier(jnp.sum(onehot, axis=0))
    perturb = adv_init * init_noise
    grads_in = jnp.zeros((D, FF), jnp.float32)
    grads_out = jnp.zeros((FF, D), jnp.float32)
    for ascent in range(ASCENTS):
        embedded = tokens.astype(jnp.float32) + perturb
        emb_bf = lax.optimization_barrier(embedded.astype(jnp.bfloat16))
        emb_float = emb_bf.astype(jnp.float32)
        inv_rms = lax.rsqrt(lax.optimization_barrier(jnp.mean(emb_float * emb_float, axis=1, keepdims=True)) + 1e-06)
        normed = (emb_float * inv_rms * norm_gain).astype(jnp.bfloat16)

        def forward(running, weights):
            preact = jnp.dot(normed, weights[0], preferred_element_type=jnp.float32)
            hidden = gelu_value(preact).astype(jnp.bfloat16)
            return (running + jnp.dot(hidden, weights[1], preferred_element_type=jnp.float32), None)
        mixed, _ = lax.scan(forward, jnp.zeros((TOKENS, D), jnp.float32), (weights_in, weights_out))
        out_grad = (embedded + mixed - target) * loss_scale
        grad_bf = out_grad.astype(jnp.bfloat16)

        def backward(running, weights):
            preact = jnp.dot(normed, weights[0], preferred_element_type=jnp.float32)
            hidden = gelu_value(preact).astype(jnp.bfloat16)
            hidden_grad = (jnp.dot(grad_bf, weights[1].T, preferred_element_type=jnp.float32) * gelu_slope(preact)).astype(jnp.bfloat16)
            part_in = jnp.dot(normed.T, hidden_grad, preferred_element_type=jnp.float32)
            part_out = jnp.dot(hidden.T, grad_bf, preferred_element_type=jnp.float32)
            running = running + jnp.dot(hidden_grad, weights[0].T, preferred_element_type=jnp.float32)
            return (running, (part_in, part_out))
        normed_grad, (parts_in, parts_out) = lax.scan(backward, jnp.zeros((TOKENS, D), jnp.float32), (weights_in, weights_out))
        grads_in = grads_in + parts_in.transpose(1, 0, 2).reshape(D, FF)
        grads_out = grads_out + parts_out.reshape(FF, D)
        if ascent + 1 < ASCENTS:
            scaled = normed_grad * norm_gain
            row_dot = lax.optimization_barrier(jnp.sum(scaled * emb_float, axis=1, keepdims=True))
            delta_grad = out_grad + inv_rms * scaled - emb_float * inv_rms * inv_rms * inv_rms * row_dot / D
            row_squares = lax.optimization_barrier(jnp.sum(delta_grad * delta_grad, axis=1))
            square_sums = lax.optimization_barrier(jnp.sum(onehot * row_squares[:, None], axis=0))
            root_mean = jnp.sqrt(square_sums / (counts * D) + 1e-06)
            token_scale = lax.optimization_barrier(jnp.sum(onehot * (adv_step / root_mean)[None, :], axis=1))
            perturb = perturb + delta_grad * token_scale[:, None]
    new_moment_in = decay * moment_in + grads_in / ASCENTS
    new_moment_out = decay * moment_out + grads_out / ASCENTS
    new_weight_in = (weight_in.astype(jnp.float32) - learn_rate * new_moment_in).astype(jnp.bfloat16)
    new_weight_out = (weight_out.astype(jnp.float32) - learn_rate * new_moment_out).astype(jnp.bfloat16)
    return (new_weight_in, new_weight_out, new_moment_in, new_moment_out, perturb)
```

```python
import functools

import jax
import jax.numpy as jnp
from jax import lax
from jax.experimental import pallas as pl
from jax.experimental.pallas import tpu as pltpu
from jax.sharding import PartitionSpec as P

ASCENTS = 2

coeff = 0.7978845608
adv_init = 0.5
adv_step = 0.5
decay = 0.9
learn_rate = 0.01


def gelu_both(values):
    square = values * values
    tangent = jnp.tanh(coeff * (values + 0.044715 * square * values))
    half = 0.5 * (1.0 + tangent)
    slope = half + 0.5 * values * (1.0 - tangent * tangent) * coeff * (1.0 + 3.0 * 0.044715 * square)
    return values * half, slope


class Place:
    def __init__(self):
        self.dp_count, self.tensor_count = lax.axis_size("dp"), lax.axis_size("tensor")
        self.ys, self.zs = self.dp_count // 2, self.tensor_count // 2
        self.dp, self.tensor = lax.axis_index("dp"), lax.axis_index("tensor")
        self.y, self.core = self.dp // 2, self.dp % 2
        self.z, self.x = self.tensor // 2, self.tensor % 2


def enter(at):
    barrier = pltpu.get_barrier_semaphore()
    for step in range(1, at.tensor_count):
        there = (at.dp, lax.rem(at.tensor + step, at.tensor_count))
        pl.semaphore_signal(barrier, inc=1, device_id=there, device_id_type=pl.DeviceIdType.MESH)
    for step in range(1, at.dp_count):
        there = (lax.rem(at.dp + step, at.dp_count), at.tensor)
        pl.semaphore_signal(barrier, inc=1, device_id=there, device_id_type=pl.DeviceIdType.MESH)
    pl.semaphore_wait(barrier, at.tensor_count + at.dp_count - 2)


def send(source, target, sems, number, there):
    copy = pltpu.make_async_remote_copy(
        src_ref=source,
        dst_ref=target,
        send_sem=sems[0].at[number],
        recv_sem=sems[1].at[number],
        device_id=there,
        device_id_type=pl.DeviceIdType.MESH,
    )
    copy.start()
    return copy


def gather_copies(dp_count, tensor_count):
    zs, ys = tensor_count // 2, dp_count // 2
    return (zs - 1) + zs + 2 * zs * (ys - 1) + 2 * zs * ys


def gather(at, own_ref, whole_ref, sems):
    rows, cols = own_ref.shape
    numbers = iter(range(gather_copies(at.dp_count, at.tensor_count)))
    started, to_core = [], []

    def place(dp, tensor):
        span = pl.ds(pl.multiple_of(dp * rows, rows), rows)
        if len(whole_ref.shape) == 3:
            return (tensor, span)
        return (span, pl.ds(pl.multiple_of(tensor * cols, cols), cols))

    def block(dp, tensor):
        return whole_ref.at[place(dp, tensor)]

    def start(source, dp, tensor, there):
        copy = send(source, block(dp, tensor), sems, next(numbers), there)
        started.append(copy)
        return copy

    def share(source, dp, tensor):
        to_core.append(start(source, dp, tensor, (at.y * 2 + 1 - at.core, at.tensor)))

    other_x = (at.dp, at.z * 2 + 1 - at.x)
    along_z = {
        k: start(
            own_ref, at.dp, at.tensor, (at.dp, lax.rem(at.z + at.zs - k, at.zs) * 2 + at.x)
        )
        for k in range(1, at.zs)
    }
    whole_ref[place(at.dp, at.tensor)] = own_ref[...]
    along_x, along_y, corner = {}, {}, {}
    column = [lax.rem(at.z + k, at.zs) * 2 for k in range(at.zs)]
    line = [lax.rem(at.y + j, at.ys) * 2 + at.core for j in range(at.ys)]
    back = [lax.rem(at.y + at.ys - j, at.ys) * 2 + at.core for j in range(at.ys)]
    for k in range(at.zs):
        mine = column[k] + at.x
        source = own_ref
        if k:
            along_z[k].wait_recv()
            source = block(at.dp, mine)
        along_x[k] = start(source, at.dp, mine, other_x)
        for j in range(1, at.ys):
            along_y[k, j] = start(source, at.dp, mine, (back[j], at.tensor))
        share(source, at.dp, mine)
    for k in range(at.zs):
        mine, beside = column[k] + at.x, column[k] + 1 - at.x
        along_x[k].wait_recv()
        for j in range(1, at.ys):
            if k % 2 == 0:
                corner[k, j] = start(
                    block(at.dp, beside), at.dp, beside, (back[j], at.tensor)
                )
        share(block(at.dp, beside), at.dp, beside)
        for j in range(1, at.ys):
            along_y[k, j].wait_recv()
            if k % 2 == 1:
                corner[k, j] = start(block(line[j], mine), line[j], mine, other_x)
            share(block(line[j], mine), line[j], mine)
    for k in range(at.zs):
        beside = column[k] + 1 - at.x
        for j in range(1, at.ys):
            corner[k, j].wait_recv()
            share(block(line[j], beside), line[j], beside)
    for copy in to_core:
        copy.wait_recv()
    for copy in started:
        copy.wait_send()


def scatter_sum(at, partial_ref, landing, sems):
    cols = landing.shape[2]

    def own(tensor):
        if len(partial_ref.shape) == 3:
            return (tensor,)
        return (slice(None), pl.ds(pl.multiple_of(tensor * cols, cols), cols))

    copies = []
    for step in range(1, at.tensor_count):
        there = lax.rem(at.tensor + step, at.tensor_count)
        copies.append(
            send(
                partial_ref.at[own(there)], landing.at[step - 1], sems, step - 1, (at.dp, there)
            )
        )
    value = partial_ref[own(at.tensor)].astype(jnp.float32)
    for step, copy in enumerate(copies):
        copy.wait_recv()
        value = value + landing[step].astype(jnp.float32)
    for copy in copies:
        copy.wait_send()
    return value


def first_kernel(emb_ref, whole_ref, *sems):
    at = Place()
    enter(at)
    gather(at, emb_ref, whole_ref, sems)


def forward_kernel(
    partial_ref, tokens_ref, perturb_ref, target_ref, whole_ref, out_grad_ref,
    landing, own, send_sum, recv_sum, send_all, recv_all, *, scale,
):
    at = Place()
    enter(at)
    mixed = scatter_sum(at, partial_ref, landing, (send_sum, recv_sum))
    embedded = tokens_ref[...].astype(jnp.float32) + perturb_ref[...]
    out_grad = (embedded + mixed - target_ref[...]) * scale
    own[...] = out_grad.astype(jnp.bfloat16)
    out_grad_ref[...] = out_grad
    gather(at, own, whole_ref, (send_all, recv_all))


def ascent_kernel(
    partial_ref, tokens_ref, perturb_ref, out_grad_ref, inv_ref, gain_ref, ids_ref,
    whole_ref, new_ref,
    landing, own, stats, stats_in, squares, squares_in,
    send_sum, recv_sum, send_stat, recv_stat, send_square, recv_square, send_all, recv_all,
    *, features,
):
    at = Place()
    enter(at)
    rows = own.shape[0]
    examples = squares.shape[0] // 2
    scaled = gain_ref[...] * scatter_sum(at, partial_ref, landing, (send_sum, recv_sum))
    tokens = tokens_ref[...].astype(jnp.float32)
    perturb = perturb_ref[...]
    emb = (tokens + perturb).astype(jnp.bfloat16).astype(jnp.float32)
    inv = inv_ref[...]
    base = out_grad_ref[...] + inv * scaled
    radial = emb * (inv * inv * inv * (1.0 / features))
    lane = lax.broadcasted_iota(jnp.int32, (rows, rows), 1)
    table = jnp.where(lane == 0, jnp.sum(scaled * emb, axis=1, keepdims=True), 0.0)
    table = jnp.where(lane == 1, jnp.sum(base * base, axis=1, keepdims=True), table)
    table = jnp.where(lane == 2, jnp.sum(base * radial, axis=1, keepdims=True), table)
    table = jnp.where(lane == 3, jnp.sum(radial * radial, axis=1, keepdims=True), table)
    own_stats = table.T[:8, :]
    stats[...] = own_stats
    copies = [
        send(
            stats, stats_in.at[step - 1], (send_stat, recv_stat), step - 1,
            (at.dp, lax.rem(at.tensor + step, at.tensor_count)),
        )
        for step in range(1, at.tensor_count)
    ]
    summed = own_stats
    for step, copy in enumerate(copies):
        copy.wait_recv()
        summed = summed + stats_in[step]
    for copy in copies:
        copy.wait_send()
    row_dot = summed[0:1, :]
    row_squares = (
        summed[1:2, :] - 2.0 * row_dot * summed[2:3, :] + row_dot * row_dot * summed[3:4, :]
    )
    label = lax.broadcasted_iota(jnp.int32, (examples, rows), 0)
    onehot = (label == ids_ref[...]).astype(jnp.float32)
    local = jnp.concatenate(
        [
            jnp.broadcast_to(
                jnp.sum(onehot * row_squares, axis=1, keepdims=True), (examples, rows)
            ),
            jnp.broadcast_to(jnp.sum(onehot, axis=1, keepdims=True), (examples, rows)),
        ],
        axis=0,
    )
    squares[...] = local
    copies = [
        send(
            squares, squares_in.at[step - 1], (send_square, recv_square), step - 1,
            (lax.rem(at.dp + step, at.dp_count), at.tensor),
        )
        for step in range(1, at.dp_count)
    ]
    for step, copy in enumerate(copies):
        copy.wait_recv()
        local = local + squares_in[step]
    for copy in copies:
        copy.wait_send()
    square_sums, counts = jnp.maximum(local[:examples], 0.0), local[examples:]
    root_mean = jnp.sqrt(square_sums / (jnp.maximum(counts, 1.0) * features) + 1e-06)
    token_scale = jnp.sum(onehot * (adv_step / root_mean), axis=0, keepdims=True)
    high = lax.broadcasted_iota(jnp.int32, (rows, rows), 0)
    columns = jnp.where(high == 0, token_scale, jnp.where(high == 1, row_dot, 0.0)).T
    perturb = perturb + (base - radial * columns[:, 1:2]) * columns[:, 0:1]
    new_ref[...] = perturb
    own[...] = (tokens + perturb).astype(jnp.bfloat16)
    gather(at, own, whole_ref, (send_all, recv_all))


def talk(kernel, number, out_shape, scratch, *args):
    vmem = pl.BlockSpec(memory_space=pltpu.VMEM)
    return pl.pallas_call(
        kernel,
        name=f"talk{number}",
        out_shape=out_shape,
        in_specs=[vmem] * len(args),
        out_specs=jax.tree.map(lambda _: vmem, out_shape),
        scratch_shapes=scratch,
        compiler_params=pltpu.CompilerParams(collective_id=number, has_side_effects=True),
    )(*args)


def shards(
    tokens, init_noise, segment_ids, target, norm_gain, weight_in, weight_out, moment_in, moment_out
):
    dp_count, tensor_count = lax.axis_size("dp"), lax.axis_size("tensor")
    rows, width = tokens.shape
    features = weight_in.shape[0]
    loss_scale = (rows * dp_count) ** (-0.5)
    me = lax.axis_index("dp")
    own_rows = moment_in.shape[0]
    examples = 2 * dp_count
    gain_own = lax.dynamic_slice_in_dim(norm_gain, lax.axis_index("tensor") * width, width, 0)
    dma = pltpu.SemaphoreType.DMA
    copies = gather_copies(dp_count, tensor_count)
    gather_sems = [dma((copies,)), dma((copies,))]
    sum_sems = [dma((tensor_count - 1,)), dma((tensor_count - 1,))]
    square_sems = [dma((dp_count - 1,)), dma((dp_count - 1,))]
    landing = pltpu.VMEM((tensor_count - 1, rows, width), jnp.bfloat16)
    own_block = pltpu.VMEM((rows, width), jnp.bfloat16)
    narrow = width % 128 != 0
    total = rows * dp_count
    whole = jax.ShapeDtypeStruct(
        (tensor_count, total, width) if narrow else (total, features), jnp.bfloat16
    )

    def flat(array):
        return array.transpose(1, 0, 2).reshape(total, features) if narrow else array

    def split(array):
        return array.reshape(rows, tensor_count, width).transpose(1, 0, 2) if narrow else array

    block = jax.ShapeDtypeStruct((rows, width), jnp.float32)
    perturb = adv_init * init_noise
    emb_bf = (tokens.astype(jnp.float32) + perturb).astype(jnp.bfloat16)
    gathered_bf = talk(first_kernel, 0, whole, gather_sems, emb_bf)
    grad_in = jnp.zeros(moment_in.shape, jnp.float32)
    grad_out = jnp.zeros(moment_out.shape, jnp.float32)
    for ascent in range(ASCENTS):
        gathered = flat(gathered_bf).astype(jnp.float32)
        inv_rms = lax.rsqrt(jnp.mean(gathered * gathered, axis=1, keepdims=True) + 1e-06)
        normed = (gathered * inv_rms * norm_gain).astype(jnp.bfloat16)
        preact = jnp.dot(normed, weight_in, preferred_element_type=jnp.float32)
        hidden, slope = gelu_both(preact)
        hidden = hidden.astype(jnp.bfloat16)
        hidden_own = lax.dynamic_slice_in_dim(hidden, me * rows, rows, 0)
        partial_value = jnp.dot(
            hidden_own, weight_out, preferred_element_type=jnp.float32
        ).astype(jnp.bfloat16)
        grad_whole, out_grad = talk(
            functools.partial(forward_kernel, scale=loss_scale), 1 + 2 * ascent, (whole, block),
            [landing, own_block, *sum_sems, *gather_sems],
            split(partial_value), tokens, perturb, target,
        )
        grad_whole = flat(grad_whole)
        hidden_grad = (
            jnp.dot(grad_whole, weight_out.T, preferred_element_type=jnp.float32) * slope
        ).astype(jnp.bfloat16)
        if ascent + 1 < ASCENTS:
            hidden_grad_own = lax.dynamic_slice_in_dim(hidden_grad, me * rows, rows, 0)
            normed_partial = jnp.dot(
                hidden_grad_own, weight_in.T, preferred_element_type=jnp.float32
            ).astype(jnp.bfloat16)
            inv_own = lax.dynamic_slice_in_dim(inv_rms, me * rows, rows, 0)
            small = pltpu.VMEM((8, rows), jnp.float32)
            gathered_bf, perturb = talk(
                functools.partial(ascent_kernel, features=features), 2 + 2 * ascent,
                (whole, block),
                [
                    landing, own_block, small,
                    pltpu.VMEM((tensor_count - 1, 8, rows), jnp.float32),
                    pltpu.VMEM((2 * examples, rows), jnp.float32),
                    pltpu.VMEM((dp_count - 1, 2 * examples, rows), jnp.float32),
                    *sum_sems, *sum_sems, *square_sems, *gather_sems,
                ],
                split(normed_partial), tokens, perturb, out_grad, inv_own,
                gain_own.reshape(1, width), segment_ids.reshape(1, rows),
            )
        normed_cols = lax.dynamic_slice_in_dim(normed, me * own_rows, own_rows, 1)
        grad_cols = lax.dynamic_slice_in_dim(grad_whole, me * own_rows, own_rows, 1)
        grad_in = grad_in + jnp.dot(normed_cols.T, hidden_grad, preferred_element_type=jnp.float32)
        grad_out = grad_out + jnp.dot(hidden.T, grad_cols, preferred_element_type=jnp.float32)
    own_in = lax.dynamic_slice_in_dim(weight_in, me * own_rows, own_rows, 0)
    own_out = lax.dynamic_slice_in_dim(weight_out, me * own_rows, own_rows, 1)
    new_moment_in = decay * moment_in + grad_in / ASCENTS
    new_moment_out = decay * moment_out + grad_out / ASCENTS
    new_weight_in = (own_in.astype(jnp.float32) - learn_rate * new_moment_in).astype(jnp.bfloat16)
    new_weight_out = (own_out.astype(jnp.float32) - learn_rate * new_moment_out).astype(
        jnp.bfloat16
    )
    return (new_weight_in, new_weight_out, new_moment_in, new_moment_out, perturb)


def solution(mesh):
    placed = (
        P("dp", "tensor"),
        P("dp", "tensor"),
        P("dp"),
        P("dp", "tensor"),
        P(),
        P(None, "tensor"),
        P("tensor", None),
        P("dp", "tensor"),
        P("tensor", "dp"),
    )
    return jax.shard_map(
        shards,
        mesh=mesh,
        in_specs=placed,
        out_specs=(
            P("dp", "tensor"),
            P("tensor", "dp"),
            P("dp", "tensor"),
            P("tensor", "dp"),
            P("dp", "tensor"),
        ),
        check_vma=False,
    )
```

```python
import functools

import jax
import jax.numpy as jnp
from jax import lax
from jax.experimental import pallas as pl
from jax.experimental.pallas import tpu as pltpu
from jax.sharding import PartitionSpec as P

ASCENTS = 2

coeff = 0.7978845608
adv_init = 0.5
adv_step = 0.5
decay = 0.9
learn_rate = 0.01


def gelu_both(values):
    square = values * values
    tangent = jnp.tanh(coeff * (values + 0.044715 * square * values))
    half = 0.5 * (1.0 + tangent)
    slope = half + 0.5 * values * (1.0 - tangent * tangent) * coeff * (1.0 + 3.0 * 0.044715 * square)
    return values * half, slope.astype(jnp.bfloat16)


class Place:
    def __init__(self):
        self.dp_count, self.tensor_count = lax.axis_size("dp"), lax.axis_size("tensor")
        self.ys, self.zs = self.dp_count // 2, self.tensor_count // 2
        self.dp, self.tensor = lax.axis_index("dp"), lax.axis_index("tensor")
        self.y, self.core = self.dp // 2, self.dp % 2
        self.z, self.x = self.tensor // 2, self.tensor % 2


def enter(at):
    barrier = pltpu.get_barrier_semaphore()
    for step in range(1, at.tensor_count):
        there = (at.dp, lax.rem(at.tensor + step, at.tensor_count))
        pl.semaphore_signal(barrier, inc=1, device_id=there, device_id_type=pl.DeviceIdType.MESH)
    for step in range(1, at.dp_count):
        there = (lax.rem(at.dp + step, at.dp_count), at.tensor)
        pl.semaphore_signal(barrier, inc=1, device_id=there, device_id_type=pl.DeviceIdType.MESH)
    pl.semaphore_wait(barrier, at.tensor_count + at.dp_count - 2)


def send(source, target, sems, number, there):
    copy = pltpu.make_async_remote_copy(
        src_ref=source,
        dst_ref=target,
        send_sem=sems[0].at[number],
        recv_sem=sems[1].at[number],
        device_id=there,
        device_id_type=pl.DeviceIdType.MESH,
    )
    copy.start()
    return copy


def gather_copies(dp_count, tensor_count):
    zs, ys = tensor_count // 2, dp_count // 2
    return (zs - 1) + zs + 2 * zs * (ys - 1) + 2 * zs * ys


def gather(at, own_ref, whole_ref, sems):
    rows, cols = own_ref.shape
    numbers = iter(range(gather_copies(at.dp_count, at.tensor_count)))
    started, to_core = [], []

    def place(dp, tensor):
        span = pl.ds(pl.multiple_of(dp * rows, rows), rows)
        if len(whole_ref.shape) == 3:
            return (tensor, span)
        return (span, pl.ds(pl.multiple_of(tensor * cols, cols), cols))

    def block(dp, tensor):
        return whole_ref.at[place(dp, tensor)]

    def start(source, dp, tensor, there):
        copy = send(source, block(dp, tensor), sems, next(numbers), there)
        started.append(copy)
        return copy

    def share(source, dp, tensor):
        to_core.append(start(source, dp, tensor, (at.y * 2 + 1 - at.core, at.tensor)))

    other_x = (at.dp, at.z * 2 + 1 - at.x)
    along_z = {
        k: start(
            own_ref, at.dp, at.tensor, (at.dp, lax.rem(at.z + at.zs - k, at.zs) * 2 + at.x)
        )
        for k in range(1, at.zs)
    }
    whole_ref[place(at.dp, at.tensor)] = own_ref[...]
    along_x, along_y, corner = {}, {}, {}
    column = [lax.rem(at.z + k, at.zs) * 2 for k in range(at.zs)]
    line = [lax.rem(at.y + j, at.ys) * 2 + at.core for j in range(at.ys)]
    back = [lax.rem(at.y + at.ys - j, at.ys) * 2 + at.core for j in range(at.ys)]
    for k in range(at.zs):
        mine = column[k] + at.x
        source = own_ref
        if k:
            along_z[k].wait_recv()
            source = block(at.dp, mine)
        along_x[k] = start(source, at.dp, mine, other_x)
        for j in range(1, at.ys):
            along_y[k, j] = start(source, at.dp, mine, (back[j], at.tensor))
        share(source, at.dp, mine)
    for k in range(at.zs):
        mine, beside = column[k] + at.x, column[k] + 1 - at.x
        along_x[k].wait_recv()
        for j in range(1, at.ys):
            if k % 2 == 0:
                corner[k, j] = start(
                    block(at.dp, beside), at.dp, beside, (back[j], at.tensor)
                )
        share(block(at.dp, beside), at.dp, beside)
        for j in range(1, at.ys):
            along_y[k, j].wait_recv()
            if k % 2 == 1:
                corner[k, j] = start(block(line[j], mine), line[j], mine, other_x)
            share(block(line[j], mine), line[j], mine)
    for k in range(at.zs):
        beside = column[k] + 1 - at.x
        for j in range(1, at.ys):
            corner[k, j].wait_recv()
            share(block(line[j], beside), line[j], beside)
    for copy in to_core:
        copy.wait_recv()
    for copy in started:
        copy.wait_send()


def scatter_sum(at, partial_ref, landing, sems):
    cols = landing.shape[2]

    def own(tensor):
        if len(partial_ref.shape) == 3:
            return (tensor,)
        return (slice(None), pl.ds(pl.multiple_of(tensor * cols, cols), cols))

    copies = []
    for step in range(1, at.tensor_count):
        there = lax.rem(at.tensor + step, at.tensor_count)
        copies.append(
            send(
                partial_ref.at[own(there)], landing.at[step - 1], sems, step - 1, (at.dp, there)
            )
        )
    value = partial_ref[own(at.tensor)].astype(jnp.float32)
    for step, copy in enumerate(copies):
        copy.wait_recv()
        value = value + landing[step].astype(jnp.float32)
    for copy in copies:
        copy.wait_send()
    return value


def first_kernel(emb_ref, whole_ref, *sems):
    at = Place()
    enter(at)
    gather(at, emb_ref, whole_ref, sems)


def forward_kernel(
    partial_ref, tokens_ref, perturb_ref, target_ref, whole_ref, out_grad_ref,
    landing, own, send_sum, recv_sum, send_all, recv_all, *, scale,
):
    at = Place()
    enter(at)
    mixed = scatter_sum(at, partial_ref, landing, (send_sum, recv_sum))
    embedded = tokens_ref[...].astype(jnp.float32) + perturb_ref[...]
    out_grad = (embedded + mixed - target_ref[...]) * scale
    own[...] = out_grad.astype(jnp.bfloat16)
    out_grad_ref[...] = out_grad
    gather(at, own, whole_ref, (send_all, recv_all))


def ascent_kernel(
    partial_ref, tokens_ref, perturb_ref, out_grad_ref, inv_ref, gain_ref, ids_ref,
    whole_ref, new_ref,
    landing, own, stats, stats_in, squares, squares_in,
    send_sum, recv_sum, send_stat, recv_stat, send_square, recv_square, send_all, recv_all,
    *, features,
):
    at = Place()
    enter(at)
    rows = own.shape[0]
    examples = squares.shape[0] // 2
    scaled = gain_ref[...] * scatter_sum(at, partial_ref, landing, (send_sum, recv_sum))
    tokens = tokens_ref[...].astype(jnp.float32)
    perturb = perturb_ref[...]
    emb = (tokens + perturb).astype(jnp.bfloat16).astype(jnp.float32)
    inv = inv_ref[...]
    base = out_grad_ref[...] + inv * scaled
    radial = emb * (inv * inv * inv * (1.0 / features))
    lane = lax.broadcasted_iota(jnp.int32, (rows, rows), 1)
    table = jnp.where(lane == 0, jnp.sum(scaled * emb, axis=1, keepdims=True), 0.0)
    table = jnp.where(lane == 1, jnp.sum(base * base, axis=1, keepdims=True), table)
    table = jnp.where(lane == 2, jnp.sum(base * radial, axis=1, keepdims=True), table)
    table = jnp.where(lane == 3, jnp.sum(radial * radial, axis=1, keepdims=True), table)
    own_stats = table.T[:8, :]
    stats[...] = own_stats
    copies = [
        send(
            stats, stats_in.at[step - 1], (send_stat, recv_stat), step - 1,
            (at.dp, lax.rem(at.tensor + step, at.tensor_count)),
        )
        for step in range(1, at.tensor_count)
    ]
    summed = own_stats
    for step, copy in enumerate(copies):
        copy.wait_recv()
        summed = summed + stats_in[step]
    for copy in copies:
        copy.wait_send()
    row_dot = summed[0:1, :]
    row_squares = (
        summed[1:2, :] - 2.0 * row_dot * summed[2:3, :] + row_dot * row_dot * summed[3:4, :]
    )
    label = lax.broadcasted_iota(jnp.int32, (examples, rows), 0)
    onehot = (label == ids_ref[...]).astype(jnp.float32)
    local = jnp.concatenate(
        [
            jnp.broadcast_to(
                jnp.sum(onehot * row_squares, axis=1, keepdims=True), (examples, rows)
            ),
            jnp.broadcast_to(jnp.sum(onehot, axis=1, keepdims=True), (examples, rows)),
        ],
        axis=0,
    )
    squares[...] = local
    copies = [
        send(
            squares, squares_in.at[step - 1], (send_square, recv_square), step - 1,
            (lax.rem(at.dp + step, at.dp_count), at.tensor),
        )
        for step in range(1, at.dp_count)
    ]
    for step, copy in enumerate(copies):
        copy.wait_recv()
        local = local + squares_in[step]
    for copy in copies:
        copy.wait_send()
    square_sums, counts = jnp.maximum(local[:examples], 0.0), local[examples:]
    root_mean = jnp.sqrt(square_sums / (jnp.maximum(counts, 1.0) * features) + 1e-06)
    token_scale = jnp.sum(onehot * (adv_step / root_mean), axis=0, keepdims=True)
    high = lax.broadcasted_iota(jnp.int32, (rows, rows), 0)
    columns = jnp.where(high == 0, token_scale, jnp.where(high == 1, row_dot, 0.0)).T
    perturb = perturb + (base - radial * columns[:, 1:2]) * columns[:, 0:1]
    new_ref[...] = perturb
    own[...] = (tokens + perturb).astype(jnp.bfloat16)
    gather(at, own, whole_ref, (send_all, recv_all))


def talk(kernel, number, out_shape, scratch, *args):
    vmem = pl.BlockSpec(memory_space=pltpu.VMEM)
    return pl.pallas_call(
        kernel,
        name=f"talk{number}",
        out_shape=out_shape,
        in_specs=[vmem] * len(args),
        out_specs=jax.tree.map(lambda _: vmem, out_shape),
        scratch_shapes=scratch,
        compiler_params=pltpu.CompilerParams(collective_id=number, has_side_effects=True),
    )(*args)


def shards(
    tokens, init_noise, segment_ids, target, norm_gain, weight_in, weight_out, moment_in, moment_out
):
    dp_count, tensor_count = lax.axis_size("dp"), lax.axis_size("tensor")
    rows, width = tokens.shape
    features = weight_in.shape[0]
    loss_scale = (rows * dp_count) ** (-0.5)
    me = lax.axis_index("dp")
    own_rows = moment_in.shape[0]
    examples = 2 * dp_count
    gain_own = lax.dynamic_slice_in_dim(norm_gain, lax.axis_index("tensor") * width, width, 0)
    dma = pltpu.SemaphoreType.DMA
    copies = gather_copies(dp_count, tensor_count)
    gather_sems = [dma((copies,)), dma((copies,))]
    sum_sems = [dma((tensor_count - 1,)), dma((tensor_count - 1,))]
    square_sems = [dma((dp_count - 1,)), dma((dp_count - 1,))]
    landing = pltpu.VMEM((tensor_count - 1, rows, width), jnp.bfloat16)
    own_block = pltpu.VMEM((rows, width), jnp.bfloat16)
    narrow = width % 128 != 0
    total = rows * dp_count
    whole = jax.ShapeDtypeStruct(
        (tensor_count, total, width) if narrow else (total, features), jnp.bfloat16
    )

    def flat(array):
        return array.transpose(1, 0, 2).reshape(total, features) if narrow else array

    def split(array):
        return array.reshape(rows, tensor_count, width).transpose(1, 0, 2) if narrow else array

    block = jax.ShapeDtypeStruct((rows, width), jnp.float32)
    perturb = adv_init * init_noise
    emb_bf = (tokens.astype(jnp.float32) + perturb).astype(jnp.bfloat16)
    gathered_bf = talk(first_kernel, 0, whole, gather_sems, emb_bf)
    grad_in = jnp.zeros(moment_in.shape, jnp.float32)
    grad_out = jnp.zeros(moment_out.shape, jnp.float32)
    for ascent in range(ASCENTS):
        gathered = flat(gathered_bf).astype(jnp.float32)
        inv_rms = lax.rsqrt(jnp.mean(gathered * gathered, axis=1, keepdims=True) + 1e-06)
        normed = (gathered * inv_rms * norm_gain).astype(jnp.bfloat16)
        preact = jnp.dot(normed, weight_in, preferred_element_type=jnp.float32)
        hidden, slope = gelu_both(preact)
        hidden = hidden.astype(jnp.bfloat16)
        hidden_own = lax.dynamic_slice_in_dim(hidden, me * rows, rows, 0)
        partial_value = jnp.dot(
            hidden_own, weight_out, preferred_element_type=jnp.float32
        ).astype(jnp.bfloat16)
        grad_whole, out_grad = talk(
            functools.partial(forward_kernel, scale=loss_scale), 1 + 2 * ascent, (whole, block),
            [landing, own_block, *sum_sems, *gather_sems],
            split(partial_value), tokens, perturb, target,
        )
        grad_whole = flat(grad_whole)
        hidden_grad = (
            jnp.dot(grad_whole, weight_out.T, preferred_element_type=jnp.float32) * slope
        ).astype(jnp.bfloat16)
        if ascent + 1 < ASCENTS:
            hidden_grad_own = lax.dynamic_slice_in_dim(hidden_grad, me * rows, rows, 0)
            normed_partial = jnp.dot(
                hidden_grad_own, weight_in.T, preferred_element_type=jnp.float32
            ).astype(jnp.bfloat16)
            inv_own = lax.dynamic_slice_in_dim(inv_rms, me * rows, rows, 0)
            small = pltpu.VMEM((8, rows), jnp.float32)
            gathered_bf, perturb = talk(
                functools.partial(ascent_kernel, features=features), 2 + 2 * ascent,
                (whole, block),
                [
                    landing, own_block, small,
                    pltpu.VMEM((tensor_count - 1, 8, rows), jnp.float32),
                    pltpu.VMEM((2 * examples, rows), jnp.float32),
                    pltpu.VMEM((dp_count - 1, 2 * examples, rows), jnp.float32),
                    *sum_sems, *sum_sems, *square_sems, *gather_sems,
                ],
                split(normed_partial), tokens, perturb, out_grad, inv_own,
                gain_own.reshape(1, width), segment_ids.reshape(1, rows),
            )
        normed_cols = lax.dynamic_slice_in_dim(normed, me * own_rows, own_rows, 1)
        grad_cols = lax.dynamic_slice_in_dim(grad_whole, me * own_rows, own_rows, 1)
        grad_in = grad_in + jnp.dot(normed_cols.T, hidden_grad, preferred_element_type=jnp.float32)
        grad_out = grad_out + jnp.dot(hidden.T, grad_cols, preferred_element_type=jnp.float32)
    own_in = lax.dynamic_slice_in_dim(weight_in, me * own_rows, own_rows, 0)
    own_out = lax.dynamic_slice_in_dim(weight_out, me * own_rows, own_rows, 1)
    new_moment_in = decay * moment_in + grad_in / ASCENTS
    new_moment_out = decay * moment_out + grad_out / ASCENTS
    new_weight_in = (own_in.astype(jnp.float32) - learn_rate * new_moment_in).astype(jnp.bfloat16)
    new_weight_out = (own_out.astype(jnp.float32) - learn_rate * new_moment_out).astype(
        jnp.bfloat16
    )
    return (new_weight_in, new_weight_out, new_moment_in, new_moment_out, perturb)


def solution(mesh):
    placed = (
        P("dp", "tensor"),
        P("dp", "tensor"),
        P("dp"),
        P("dp", "tensor"),
        P(),
        P(None, "tensor"),
        P("tensor", None),
        P("dp", "tensor"),
        P("tensor", "dp"),
    )
    return jax.shard_map(
        shards,
        mesh=mesh,
        in_specs=placed,
        out_specs=(
            P("dp", "tensor"),
            P("tensor", "dp"),
            P("dp", "tensor"),
            P("tensor", "dp"),
            P("dp", "tensor"),
        ),
        check_vma=False,
    )
```
